16 devices in a mesh: cp: 2 (over z), fsdp: 8 (over y, x, core).
Axes of the slice: x: 2, y: 2, z: 2, core: 2. Of those that a mesh axis runs over, the one named last changes fastest.
Arguments:
- x_in: bfloat16 [8, 4096, 1152], P('fsdp', 'cp')
- grad_out: bfloat16 [8, 4096, 1152], P('fsdp', 'cp')
- seg_id: int32 [8, 4096], P('fsdp', 'cp')
- seg_pos: int32 [8, 4096], P('fsdp', 'cp')
- norm_scale: float32 [1152], P(('cp', 'fsdp'))
- w_q: float32 [1152, 1024], P(('cp', 'fsdp'))
- w_k: float32 [1152, 256], P(('cp', 'fsdp'))
- w_v: float32 [1152, 256], P(('cp', 'fsdp'))
- w_o: float32 [1024, 1152], P(('cp', 'fsdp'))
- b_o: float32 [1152], P(('cp', 'fsdp'))
- w_up1: float32 [1152, 6912], P(('cp', 'fsdp'))
- b_up1: float32 [6912], P(('cp', 'fsdp'))
- w_up2: float32 [1152, 6912], P(('cp', 'fsdp'))
- b_up2: float32 [6912], P(('cp', 'fsdp'))
- w_down: float32 [6912, 1152], P(('cp', 'fsdp'))
- b_down: float32 [1152], P(('cp', 'fsdp'))
Outputs:
- output 1: bfloat16 [8, 4096, 1152], P('fsdp', 'cp')
- output 2: bfloat16 [8, 4096, 1152], P('fsdp', 'cp')
- output 3: float32 [1152], P(('cp', 'fsdp'))
- output 4: float32 [1152, 1024], P(('cp', 'fsdp'))
- output 5: float32 [1152, 256], P(('cp', 'fsdp'))
- output 6: float32 [1152, 256], P(('cp', 'fsdp'))
- output 7: float32 [1024, 1152], P(('cp', 'fsdp'))
- output 8: float32 [1152], P(('cp', 'fsdp'))
- output 9: float32 [1152, 6912], P(('cp', 'fsdp'))
- output 10: float32 [6912], P(('cp', 'fsdp'))
- output 11: float32 [1152, 6912], P(('cp', 'fsdp'))
- output 12: float32 [6912], P(('cp', 'fsdp'))
- output 13: float32 [6912, 1152], P(('cp', 'fsdp'))
- output 14: float32 [1152], P(('cp', 'fsdp'))
All inputs are finite; a program needn't handle non-finite values.
Results may differ from the reference program's by a relative error of at most 0.0170754.
Values are sent between devices in bfloat16 or wider.
A program may use at most 1 GiB of HBM per device.

```python
import jax
import jax.numpy as jnp
from jax import lax

BATCH_ALL = 8
SEQ_LEN = 4096
MODEL_DIM = 1152
NUM_HEADS = 4
HEAD_DIM = 256
FFN_DIM = 6912
WINDOW = 2048
ROPE_DIMS = 128
DOC_SPREAD = 1536


def normal_draw(key, shape):
    return jax.random.normal(key, shape, jnp.float32)


def setup_inputs(seed: int = 0) -> dict:
    keys = jax.random.split(jax.random.key(seed), 16)
    qk_dim = NUM_HEADS * HEAD_DIM
    x_in = normal_draw(keys[0], (BATCH_ALL, SEQ_LEN, MODEL_DIM)).astype(jnp.bfloat16)
    grad_out = normal_draw(keys[1], (BATCH_ALL, SEQ_LEN, MODEL_DIM)).astype(jnp.bfloat16)
    positions = jnp.broadcast_to(jnp.arange(SEQ_LEN, dtype=jnp.int32), (BATCH_ALL, SEQ_LEN))
    doc_starts = (jax.random.randint(keys[2], (BATCH_ALL, SEQ_LEN), 0, DOC_SPREAD) == 0) | (positions == 0)
    seg_id = jnp.cumsum(doc_starts.astype(jnp.int32), axis=1)
    seg_pos = positions - lax.cummax(jnp.where(doc_starts, positions, 0), axis=1)
    return {
        'x_in': x_in,
        'grad_out': grad_out,
        'seg_id': seg_id,
        'seg_pos': seg_pos,
        'norm_scale': 0.3 * normal_draw(keys[3], (MODEL_DIM,)),
        'w_q': normal_draw(keys[4], (MODEL_DIM, qk_dim)) * MODEL_DIM ** -0.5,
        'w_k': normal_draw(keys[5], (MODEL_DIM, HEAD_DIM)) * MODEL_DIM ** -0.5,
        'w_v': normal_draw(keys[6], (MODEL_DIM, HEAD_DIM)) * MODEL_DIM ** -0.5,
        'w_o': normal_draw(keys[7], (qk_dim, MODEL_DIM)) * (2.0 * qk_dim ** -0.5),
        'b_o': 0.3 * normal_draw(keys[8], (MODEL_DIM,)),
        'w_up1': normal_draw(keys[9], (MODEL_DIM, FFN_DIM)) * MODEL_DIM ** -0.5,
        'b_up1': 0.5 * normal_draw(keys[10], (FFN_DIM,)),
        'w_up2': normal_draw(keys[11], (MODEL_DIM, FFN_DIM)) * MODEL_DIM ** -0.5,
        'b_up2': 0.5 * normal_draw(keys[12], (FFN_DIM,)),
        'w_down': normal_draw(keys[13], (FFN_DIM, MODEL_DIM)) * FFN_DIM ** -0.5,
        'b_down': 0.3 * normal_draw(keys[14], (MODEL_DIM,)),
    }


def bf16_value(vals):
    return vals + lax.stop_gradient(vals.astype(jnp.bfloat16).astype(jnp.float32) - vals)


def rope_apply(values, rot_angle):
    half_dims = ROPE_DIMS // 2
    cos_a = jnp.cos(rot_angle)
    sin_a = jnp.sin(rot_angle)
    first_half = values[..., :half_dims]
    second_half = values[..., half_dims:ROPE_DIMS]
    return jnp.concatenate([first_half * cos_a - second_half * sin_a, second_half * cos_a + first_half * sin_a, values[..., ROPE_DIMS:]], axis=-1)


def seq_attention(q_rot, kv_all, seg_q, seg_all):
    q_rows = min(SEQ_LEN, WINDOW // 2)
    key_span = WINDOW + q_rows
    n_blocks = SEQ_LEN // q_rows
    row_ids = jnp.arange(q_rows)[:, None]
    col_ids = jnp.arange(key_span)[None, :]
    in_window = (col_ids > row_ids) & (col_ids <= row_ids + WINDOW)

    def one_block(blk_index):
        row_start = blk_index * q_rows
        q_blk = bf16_value(lax.dynamic_slice_in_dim(q_rot, row_start, q_rows, axis=0))
        kv_blk = bf16_value(lax.dynamic_slice_in_dim(kv_all, row_start, key_span, axis=0))
        segq_blk = lax.dynamic_slice_in_dim(seg_q, row_start, q_rows, axis=0)
        segk_blk = lax.dynamic_slice_in_dim(seg_all, row_start, key_span, axis=0)
        key_pos = row_start - WINDOW + jnp.arange(key_span)
        allowed = in_window & (key_pos >= 0)[None, :] & (segq_blk[:, None] == segk_blk[None, :])
        scores = jnp.einsum('rhd,jd->hrj', q_blk, kv_blk[:, :HEAD_DIM]) * (HEAD_DIM ** -0.5)
        scores = jnp.where(allowed[None], scores, -1e30)
        scores = scores - lax.stop_gradient(jnp.max(scores, axis=-1, keepdims=True))
        exp_scores = jnp.exp(scores)
        prob_vals = bf16_value(exp_scores / jnp.sum(exp_scores, axis=-1, keepdims=True))
        return jnp.einsum('hrj,jd->rhd', prob_vals, kv_blk[:, HEAD_DIM:])

    blk_out = lax.map(jax.checkpoint(one_block), jnp.arange(n_blocks))
    return blk_out.reshape(SEQ_LEN, NUM_HEADS, HEAD_DIM)


def layer_forward(x_f, seg_id, seg_pos, weight_set):
    scale_v, wq_v, wk_v, wv_v, wo_v, bo_v, w1_v, b1_v, w2_v, b2_v, wd_v, bd_v = [bf16_value(weight_arr) for weight_arr in weight_set]
    inv_rms = lax.rsqrt(jnp.mean(x_f * x_f, axis=-1, keepdims=True) + 1e-6)
    normed = bf16_value(x_f * inv_rms * (1.0 + scale_v))
    q_lin = jnp.einsum('btd,de->bte', normed, wq_v).reshape(BATCH_ALL, SEQ_LEN, NUM_HEADS, HEAD_DIM)
    k_lin = jnp.einsum('btd,de->bte', normed, wk_v)
    v_lin = jnp.einsum('btd,de->bte', normed, wv_v)
    half_dims = ROPE_DIMS // 2
    inv_freq = 10000.0 ** (-jnp.arange(half_dims, dtype=jnp.float32) / half_dims)
    rot_angle = seg_pos.astype(jnp.float32)[..., None] * inv_freq
    q_rot = rope_apply(q_lin, rot_angle[:, :, None, :])
    kv_local = jnp.concatenate([rope_apply(k_lin, rot_angle), v_lin], axis=-1)
    kv_all = jnp.pad(kv_local, ((0, 0), (WINDOW, 0), (0, 0)))
    seg_all = jnp.pad(seg_id, ((0, 0), (WINDOW, 0)))

    def seq_item(seq_args):
        return seq_attention(seq_args[0], seq_args[1], seq_args[2], seq_args[3])

    attn_o = bf16_value(lax.map(seq_item, (q_rot, kv_all, seg_id, seg_all))).reshape(BATCH_ALL, SEQ_LEN, NUM_HEADS * HEAD_DIM)
    attn_out = jnp.einsum('bte,ed->btd', attn_o, wo_v) + bo_v
    h_one = jnp.einsum('btd,df->btf', normed, w1_v) + b1_v
    h_two = jnp.einsum('btd,df->btf', normed, w2_v) + b2_v
    act_vals = bf16_value(jax.nn.gelu(h_one, approximate=True) * h_two)
    mlp_out = jnp.einsum('btf,fd->btd', act_vals, wd_v) + bd_v
    return x_f + attn_out + mlp_out


def reference(x_in, grad_out, seg_id, seg_pos, norm_scale, w_q, w_k, w_v, w_o, b_o, w_up1, b_up1, w_up2, b_up2, w_down, b_down):
    weight_set = (norm_scale, w_q, w_k, w_v, w_o, b_o, w_up1, b_up1, w_up2, b_up2, w_down, b_down)

    def forward(x_f, weights_in):
        return layer_forward(x_f, seg_id, seg_pos, weights_in)

    out_f, pullback = jax.vjp(forward, x_in.astype(jnp.float32), weight_set)
    d_xf, d_set = pullback(grad_out.astype(jnp.float32))
    return (out_f.astype(jnp.bfloat16), d_xf.astype(jnp.bfloat16), d_set[0], d_set[1], d_set[2], d_set[3], d_set[4], d_set[5], d_set[6], d_set[7], d_set[8], d_set[9], d_set[10], d_set[11])
```

```python
import functools
import jax
import jax.numpy as jnp
from jax import lax
from jax.experimental import pallas as pl
from jax.experimental.layout import Layout, with_layout_constraint
from jax.experimental.pallas import tpu as pltpu
from jax.sharding import PartitionSpec as P

WINDOW = 2048
ROPE_DIMS = 128
PARAM_AXES = ('cp', 'fsdp')
BQ = 256
BK = 256
FT = 256
VMEM_BYTES = 62 * 1024 * 1024
GELU_C = 0.7978845608028654
GELU_A = 0.044715


def rope_angle(seg_pos):
    half_dims = ROPE_DIMS // 2
    inv_freq = 10000.0 ** (-jnp.arange(half_dims, dtype=jnp.float32) / half_dims)
    return seg_pos.astype(jnp.float32)[..., None] * inv_freq


def rope_apply(values, cos_a, sin_a):
    half_dims = ROPE_DIMS // 2
    first_half = values[..., :half_dims]
    second_half = values[..., half_dims:ROPE_DIMS]
    return jnp.concatenate([first_half * cos_a - second_half * sin_a, second_half * cos_a + first_half * sin_a, values[..., ROPE_DIMS:]], axis=-1)


def rms_norm(x_f, scale_f):
    inv_rms = lax.rsqrt(jnp.mean(x_f * x_f, axis=-1, keepdims=True) + 1e-6)
    return x_f * inv_rms * (1.0 + scale_f)


def resident(shape):
    return pl.BlockSpec(shape, lambda *_: (0,) * len(shape), pipeline_mode=pl.Buffered(1))


def attn_kernel(n_heads, head_dim, lo_ref, q_ref, do_ref, cos_ref, sin_ref, kv_ref, kvt_ref, segk_ref, segq_ref, o_ref, dq_ref, dprev_ref, down_ref, q4, qt, do4, dot_, s_scr, dp_scr, dkv_ref):
    qb = pl.program_id(0)
    scale = head_dim ** -0.5
    cos_a = cos_ref[...]
    sin_a = sin_ref[...]

    def turn(vals, cos_v, sin_v):
        front = vals[:, :ROPE_DIMS]
        return jnp.concatenate([front * cos_v + pltpu.roll(front, ROPE_DIMS // 2, 1) * sin_v, vals[:, ROPE_DIMS:]], axis=1)

    @pl.when(qb == 0)
    def _():
        dkv_ref[...] = jnp.zeros_like(dkv_ref)

    for h in range(n_heads):
        cols = slice(h * head_dim, (h + 1) * head_dim)
        rows = slice(h * BQ, (h + 1) * BQ)
        q_f = turn(q_ref[:, cols], cos_a, sin_a)
        q_h = q_f.astype(jnp.bfloat16)
        do_h = do_ref[:, cols]
        q4[rows, :] = q_h
        do4[rows, :] = do_h
        qt[:, rows] = q_f.T.astype(jnp.bfloat16)
        dot_[:, rows] = do_h.astype(jnp.float32).T.astype(jnp.bfloat16)

    lo = lo_ref[qb]
    hi = (qb * BQ + BQ - 1 + WINDOW) // BK + 1
    segq = segq_ref[0]
    gap = lax.broadcasted_iota(jnp.int32, (BK, BQ), 1) - lax.broadcasted_iota(jnp.int32, (BK, BQ), 0)

    def k_rows(kb):
        return pl.ds(pl.multiple_of(kb * BK, BK), BK)

    def scores_step(kb, m):
        k_blk = kv_ref[k_rows(kb), :head_dim]
        dist = gap + (qb * BQ + WINDOW - kb * BK)
        allowed = (segk_ref[k_rows(kb), :] == segq) & (dist >= 0) & (dist < WINDOW)
        parts = []
        for h in range(n_heads):
            rows = slice(h * BQ, (h + 1) * BQ)
            s_h = jnp.dot(k_blk, qt[:, rows], preferred_element_type=jnp.float32) * scale
            s_h = jnp.where(allowed, s_h, -1e30)
            s_scr[kb - lo, :, rows] = s_h
            parts.append(jnp.maximum(m[h], jnp.max(s_h, axis=0, keepdims=True)))
        return tuple(parts)

    m = lax.fori_loop(lo, hi, scores_step, tuple(jnp.full((1, BQ), -1e30, jnp.float32) for _ in range(n_heads)))

    def exp_step(kb, carry):
        v_blk = kv_ref[k_rows(kb), head_dim:]
        sums, dots = [], []
        for h in range(n_heads):
            rows = slice(h * BQ, (h + 1) * BQ)
            dp_h = jnp.dot(v_blk, dot_[:, rows], preferred_element_type=jnp.float32)
            p_h = jnp.exp(s_scr[kb - lo, :, rows] - m[h])
            s_scr[kb - lo, :, rows] = p_h
            dp_scr[kb - lo, :, rows] = dp_h
            sums.append(carry[0][h] + jnp.sum(p_h, axis=0, keepdims=True))
            dots.append(carry[1][h] + jnp.sum(p_h * dp_h, axis=0, keepdims=True))
        return tuple(sums), tuple(dots)

    zeros = tuple(jnp.zeros((1, BQ), jnp.float32) for _ in range(n_heads))
    sums, dots = lax.fori_loop(lo, hi, exp_step, (zeros, zeros))
    inv_sum = [1.0 / sums[h] for h in range(n_heads)]
    delta = [dots[h] * inv_sum[h] for h in range(n_heads)]

    def grad_step(kb, carry):
        o_acc, dq_acc = carry
        cols = pl.ds(pl.multiple_of(kb * BK, BK), BK)
        kt_blk = kvt_ref[:head_dim, cols]
        vt_blk = kvt_ref[head_dim:, cols]
        p_parts, ds_parts = [], []
        for h in range(n_heads):
            rows = slice(h * BQ, (h + 1) * BQ)
            p_h = s_scr[kb - lo, :, rows] * inv_sum[h]
            ds_h = p_h * (dp_scr[kb - lo, :, rows] - delta[h]) * scale
            p_parts.append(p_h.astype(jnp.bfloat16))
            ds_parts.append(ds_h.astype(jnp.bfloat16))
        p_all = jnp.concatenate(p_parts, axis=1)
        ds_all = jnp.concatenate(ds_parts, axis=1)
        dkv_ref[k_rows(kb), :head_dim] += jnp.dot(ds_all, q4[...], preferred_element_type=jnp.float32)
        dkv_ref[k_rows(kb), head_dim:] += jnp.dot(p_all, do4[...], preferred_element_type=jnp.float32)
        o_acc = o_acc + jnp.dot(vt_blk, p_all, preferred_element_type=jnp.float32)
        dq_acc = dq_acc + jnp.dot(kt_blk, ds_all, preferred_element_type=jnp.float32)
        return o_acc, dq_acc

    wide = jnp.zeros((head_dim, n_heads * BQ), jnp.float32)
    o_acc, dq_acc = lax.fori_loop(lo, hi, grad_step, (wide, wide))
    for h in range(n_heads):
        cols = slice(h * head_dim, (h + 1) * head_dim)
        rows = slice(h * BQ, (h + 1) * BQ)
        o_ref[:, cols] = o_acc[:, rows].T.astype(jnp.bfloat16)
        dq_ref[:, cols] = turn(dq_acc[:, rows].T, cos_a, -sin_a).astype(jnp.bfloat16)

    @pl.when(qb == pl.num_programs(0) - 1)
    def _():
        dprev_ref[...] = dkv_ref[:WINDOW, :]
        down_ref[...] = dkv_ref[WINDOW:, :]


def attention(qkv, do_b, cos_a, sin_a, kv_all, seg_q, seg_all, n_heads):
    n_tok, q_dim = do_b.shape
    head_dim = q_dim // n_heads
    n_keys = kv_all.shape[0]
    n_q = n_tok // BQ
    n_span = WINDOW // BK + BQ // BK
    seg_first = seg_q.reshape(n_q, BQ)[:, 0]
    seg_last = seg_all.reshape(n_keys // BK, BK)[:, -1]
    first_seg_blk = jnp.sum((seg_last[None, :] < seg_first[:, None]).astype(jnp.int32), axis=1)
    first_win_blk = (jnp.arange(n_q, dtype=jnp.int32) * BQ + 1) // BK
    lo_blk = jnp.maximum(first_seg_blk, first_win_blk)
    wide = n_heads * BQ
    grid_spec = pltpu.PrefetchScalarGridSpec(
        num_scalar_prefetch=1,
        grid=(n_q,),
        in_specs=[
            pl.BlockSpec((BQ, q_dim), lambda i, lo: (i, 0)),
            pl.BlockSpec((BQ, q_dim), lambda i, lo: (i, 0)),
            pl.BlockSpec((BQ, ROPE_DIMS), lambda i, lo: (i, 0)),
            pl.BlockSpec((BQ, ROPE_DIMS), lambda i, lo: (i, 0)),
            resident((n_keys, 2 * head_dim)),
            resident((2 * head_dim, n_keys)),
            resident((n_keys, 1)),
            pl.BlockSpec((1, 1, BQ), lambda i, lo: (i, 0, 0)),
        ],
        out_specs=[
            pl.BlockSpec((BQ, q_dim), lambda i, lo: (i, 0)),
            pl.BlockSpec((BQ, q_dim), lambda i, lo: (i, 0)),
            resident((WINDOW, 2 * head_dim)),
            resident((n_keys - WINDOW, 2 * head_dim)),
        ],
        scratch_shapes=[
            pltpu.VMEM((wide, head_dim), jnp.bfloat16),
            pltpu.VMEM((head_dim, wide), jnp.bfloat16),
            pltpu.VMEM((wide, head_dim), jnp.bfloat16),
            pltpu.VMEM((head_dim, wide), jnp.bfloat16),
            pltpu.VMEM((n_span, BK, wide), jnp.float32),
            pltpu.VMEM((n_span, BK, wide), jnp.float32),
            pltpu.VMEM((n_keys, 2 * head_dim), jnp.float32),
        ],
    )
    return pl.pallas_call(
        functools.partial(attn_kernel, n_heads, head_dim),
        grid_spec=grid_spec,
        out_shape=(
            jax.ShapeDtypeStruct((n_tok, q_dim), jnp.bfloat16),
            jax.ShapeDtypeStruct((n_tok, q_dim), jnp.bfloat16),
            jax.ShapeDtypeStruct((WINDOW, 2 * head_dim), jnp.float32),
            jax.ShapeDtypeStruct((n_keys - WINDOW, 2 * head_dim), jnp.float32),
        ),
        compiler_params=pltpu.CompilerParams(dimension_semantics=('arbitrary',), vmem_limit_bytes=VMEM_BYTES),
        cost_estimate=pl.CostEstimate(flops=10 * n_tok * WINDOW * q_dim, bytes_accessed=40 << 20, transcendentals=n_tok * WINDOW * n_heads),
        name='attention',
    )(lo_blk, qkv, do_b, cos_a, sin_a, kv_all, kv_all.T, seg_all.reshape(n_keys, 1), seg_q.reshape(n_q, 1, BQ))


def act_kernel(n_tok, step_rows, n_ref, g_ref, nt_ref, w1_ref, w2_ref, wd_ref, b1_ref, b2_ref, *rest):
    act_ref, dh_ref, dw_ref, db_ref, d_two_scr, db_scr = rest[-6:]

    @pl.when(pl.program_id(1) == 0)
    def _():
        def one_tile(i, sums):
            rows = pl.ds(pl.multiple_of(i * step_rows, step_rows), step_rows)
            n_blk = n_ref[rows, :]
            h_one = jnp.dot(n_blk, w1_ref[...], preferred_element_type=jnp.float32) + b1_ref[...]
            h_two = jnp.dot(n_blk, w2_ref[...], preferred_element_type=jnp.float32) + b2_ref[...]
            d_act = lax.dot_general(g_ref[rows, :], wd_ref[...], (((1,), (1,)), ((), ())), preferred_element_type=jnp.float32)
            h_sq = h_one * h_one
            t = jnp.tanh(h_one * (GELU_C + (GELU_C * GELU_A) * h_sq))
            half = 0.5 + 0.5 * t
            gelu = h_one * half
            slope = half + (0.5 * h_one) * (1.0 - t * t) * (GELU_C + (3.0 * GELU_C * GELU_A) * h_sq)
            act_ref[rows, :] = (gelu * h_two).astype(jnp.bfloat16)
            d_one = d_act * h_two * slope
            d_two = d_act * gelu
            dh_ref[rows, :] = d_one.astype(jnp.bfloat16)
            d_two_scr[rows, :] = d_two.astype(jnp.bfloat16)
            return sums[0] + jnp.sum(d_one, axis=0, keepdims=True), sums[1] + jnp.sum(d_two, axis=0, keepdims=True)

        zero = jnp.zeros((1, FT), jnp.float32)
        s_one, s_two = lax.fori_loop(0, n_tok // step_rows, one_tile, (zero, zero), unroll=2)
        db_ref[...] = s_one
        db_scr[...] = s_two
        dw_ref[...] = jnp.dot(nt_ref[...], dh_ref[...], preferred_element_type=jnp.float32)

    @pl.when(pl.program_id(1) == 1)
    def _():
        dh_ref[...] = d_two_scr[...]
        db_ref[...] = db_scr[...]
        dw_ref[...] = jnp.dot(nt_ref[...], d_two_scr[...], preferred_element_type=jnp.float32)


def act_call(normed, normed_t, grad, w12, wd, b1, b2, act_buf, first_tile, n_tiles):
    n_tok, width = normed.shape
    ffn = wd.shape[0]
    in_specs = [
        resident((n_tok, width)),
        resident((n_tok, width)),
        resident((width, n_tok)),
        pl.BlockSpec((width, FT), lambda t, k: (0, t)),
        pl.BlockSpec((width, FT), lambda t, k: (0, t + n_tiles)),
        pl.BlockSpec((FT, width), lambda t, k: (t + first_tile, 0)),
        pl.BlockSpec((1, FT), lambda t, k: (0, t + first_tile)),
        pl.BlockSpec((1, FT), lambda t, k: (0, t + first_tile)),
    ]
    args = [normed, grad, normed_t, w12, w12, wd, b1, b2]
    alias = {}
    if act_buf is not None:
        in_specs.append(pl.BlockSpec(memory_space=pl.ANY))
        alias = {len(args): 0}
        args.append(act_buf)
    return pl.pallas_call(
        functools.partial(act_kernel, n_tok, 256),
        grid=(n_tiles, 2),
        in_specs=in_specs,
        out_specs=[
            pl.BlockSpec((n_tok, FT), lambda t, k: (0, t + first_tile)),
            pl.BlockSpec((n_tok, FT), lambda t, k: (0, t + k * n_tiles)),
            pl.BlockSpec((width, FT), lambda t, k: (0, t + k * n_tiles)),
            pl.BlockSpec((1, FT), lambda t, k: (0, t + k * n_tiles)),
        ],
        out_shape=(
            jax.ShapeDtypeStruct((n_tok, ffn), jnp.bfloat16),
            jax.ShapeDtypeStruct((n_tok, n_tiles * 2 * FT), jnp.bfloat16),
            jax.ShapeDtypeStruct((width, n_tiles * 2 * FT), jnp.float32),
            jax.ShapeDtypeStruct((1, n_tiles * 2 * FT), jnp.float32),
        ),
        scratch_shapes=[pltpu.VMEM((n_tok, FT), jnp.bfloat16), pltpu.VMEM((1, FT), jnp.float32)],
        input_output_aliases=alias,
        compiler_params=pltpu.CompilerParams(dimension_semantics=('arbitrary', 'arbitrary'), vmem_limit_bytes=VMEM_BYTES),
        cost_estimate=pl.CostEstimate(flops=10 * n_tok * width * FT * n_tiles, bytes_accessed=30 << 20, transcendentals=n_tok * FT * n_tiles),
        name='gated_act',
    )(*args)


def mm(a, b):
    return jnp.dot(a, b, preferred_element_type=jnp.float32)


def mm_tn(a, b):
    return lax.dot_general(a, b, (((0,), (0,)), ((), ())), preferred_element_type=jnp.float32)


def mm_nt(a, b):
    return lax.dot_general(a, b, (((1,), (1,)), ((), ())), preferred_element_type=jnp.float32)


def solution(mesh):
    n_dev = mesh.shape['cp'] * mesh.shape['fsdp']
    tok_spec = P('fsdp', 'cp', None)
    pos_spec = P('fsdp', 'cp')
    vec_spec = P(PARAM_AXES)
    mat_spec = P(PARAM_AXES, None)
    param_specs = (vec_spec, mat_spec, mat_spec, mat_spec, mat_spec, vec_spec, mat_spec, vec_spec, mat_spec, vec_spec, mat_spec, vec_spec)
    fwd_pairs = [(0, 1)]
    back_pairs = [(1, 0)]

    def gather(piece):
        return lax.all_gather(piece, PARAM_AXES, axis=0, tiled=True)

    def scatter(full):
        return lax.psum_scatter(full, PARAM_AXES, scatter_dimension=0, tiled=True)

    def local_step(x_in, grad_out, seg_id, seg_pos, norm_scale, w_q, w_k, w_v, w_o, b_o, w_up1, b_up1, w_up2, b_up2, w_down, b_down):
        bf = jnp.bfloat16
        width = x_in.shape[2]
        head_dim = w_k.shape[1]
        q_dim = w_q.shape[1]
        n_heads = q_dim // head_dim
        ffn = w_up1.shape[1]
        n_tiles = ffn // FT
        tiles_of = (n_tiles // 3, n_tiles - n_tiles // 3)
        starts = (0, tiles_of[0])
        w_rows, f_rows, e_rows = norm_scale.shape[0], b_up1.shape[0], w_o.shape[0]

        def up_part(c):
            cols = slice(starts[c] * FT, (starts[c] + tiles_of[c]) * FT)
            return jnp.concatenate([w_up1[:, cols].astype(bf), w_up2[:, cols].astype(bf)], axis=1)

        qkv_dim = q_dim + 2 * head_dim
        vec_piece = jnp.concatenate([norm_scale, b_o, b_down, b_up1, b_up2]).astype(bf)[None]
        vec_all = gather(vec_piece).astype(jnp.float32)
        offs = [0, w_rows, 2 * w_rows, 3 * w_rows, 3 * w_rows + f_rows, 3 * w_rows + 2 * f_rows]
        scale_f, bo_f, bd_f, b1_f, b2_f = [vec_all[:, offs[i]:offs[i + 1]].reshape(1, -1) for i in range(5)]

        w12_a = gather(up_part(0))
        wd_b = gather(w_down.astype(bf))
        attn_piece = jnp.concatenate([jnp.concatenate([w_q, w_k, w_v], axis=1).astype(bf), jnp.pad(w_o.astype(bf), ((0, 0), (0, qkv_dim - width)))], axis=0)
        attn_w = gather(attn_piece).reshape(n_dev, w_rows + e_rows, qkv_dim)
        w12_b = gather(up_part(1))
        wqkv_b = attn_w[:, :w_rows].reshape(width, qkv_dim)
        wo_b = attn_w[:, w_rows:, :width].reshape(q_dim, width)

        x_f = x_in[0].astype(jnp.float32)
        grad = grad_out[0]
        grad_f = grad.astype(jnp.float32)
        normed_f, norm_back = jax.vjp(rms_norm, x_f, scale_f)
        normed = with_layout_constraint(normed_f.astype(bf), Layout((0, 1)))
        normed_t = normed.T
        d_bias = jnp.sum(grad_f, axis=0, keepdims=True)
        rot_angle = rope_angle(seg_pos[0])
        cos_h, sin_h = jnp.cos(rot_angle), jnp.sin(rot_angle)
        cos_w = jnp.concatenate([cos_h, cos_h], axis=1)
        sin_w = jnp.concatenate([-sin_h, sin_h], axis=1)

        act_a, dh_a, dw_a, db_a = act_call(normed, normed_t, grad, w12_a, wd_b, b1_f, b2_f, None, starts[0], tiles_of[0])
        dw_a_s = scatter(dw_a)

        normed_q, db_a, d_bias = lax.optimization_barrier((normed, db_a, d_bias))
        qkv = with_layout_constraint(mm(normed_q, wqkv_b), Layout((0, 1)))
        kv_b = jnp.concatenate([rope_apply(qkv[:, q_dim:q_dim + head_dim], cos_h, sin_h).astype(bf), qkv[:, q_dim + head_dim:].astype(bf)], axis=1)
        kv_prev = lax.ppermute(kv_b, 'cp', fwd_pairs)
        seg_prev = lax.ppermute(seg_id[0], 'cp', fwd_pairs)
        do_b = mm_nt(grad, wo_b).astype(bf)

        act_b, dh_b, dw_b, db_b = act_call(normed_q, normed_t, grad, w12_b, wd_b, b1_f, b2_f, act_a, starts[1], tiles_of[1])
        dw_b_s = scatter(dw_b)

        kv_all = jnp.concatenate([kv_prev, kv_b], axis=0)
        seg_all = jnp.concatenate([seg_prev, seg_id[0]], axis=0)
        qkv, db_b = lax.optimization_barrier((qkv, db_b))
        attn_o, dq_b, d_prev, d_own = attention(qkv, do_b, cos_w, sin_w, kv_all, seg_id[0], seg_all, n_heads)
        d_kvl = d_own + lax.ppermute(d_prev, 'cp', back_pairs)

        act_b, dh_a, dh_b, attn_o = lax.optimization_barrier((act_b, dh_a, dh_b, attn_o))
        dwd = mm_tn(act_b, grad)
        dwo = mm_tn(attn_o, grad)
        dkv_b = jnp.concatenate([rope_apply(d_kvl[:, :head_dim], cos_h, -sin_h).astype(bf), d_kvl[:, head_dim:].astype(bf)], axis=1)
        dqkv_b = jnp.concatenate([dq_b, dkv_b], axis=1)
        dwqkv = lax.dot_general(normed_t, dqkv_b, (((1,), (0,)), ((), ())), preferred_element_type=jnp.float32)

        def bias_rows(which):
            part_a = db_a[:, which * tiles_of[0] * FT:(which + 1) * tiles_of[0] * FT]
            part_b = db_b[:, which * tiles_of[1] * FT:(which + 1) * tiles_of[1] * FT]
            return jnp.concatenate([part_a, part_b], axis=1).reshape(n_dev, f_rows)

        vec_rows = jnp.concatenate([d_bias.reshape(n_dev, w_rows), bias_rows(0), bias_rows(1)], axis=1)
        vec_rows = jnp.pad(vec_rows[:, None], ((0, 0), (0, 31), (0, width - vec_rows.shape[1])))
        rest_dim = qkv_dim - width
        fold = width // rest_dim
        dwqkv = dwqkv.reshape(n_dev, w_rows, qkv_dim)
        rest_rows = dwqkv[:, :, width:].reshape(n_dev, fold, w_rows // fold, rest_dim)
        rest_rows = jnp.concatenate([rest_rows[:, i] for i in range(fold)], axis=2)
        last = jnp.concatenate([dwd.reshape(n_dev, f_rows, width), dwo.reshape(n_dev, e_rows, width), dwqkv[:, :, :width], rest_rows, vec_rows], axis=1)
        last_s = scatter(last.reshape(-1, width))
        last_s = lax.optimization_barrier(last_s)
        marks = [0, f_rows, f_rows + e_rows, f_rows + e_rows + w_rows, f_rows + e_rows + w_rows + w_rows // fold]
        dwd_s, d_wo, main_s, rest_s = [last_s[marks[i]:marks[i + 1]] for i in range(4)]
        rest_s = jnp.concatenate([rest_s[:, i * rest_dim:(i + 1) * rest_dim] for i in range(fold)], axis=0)
        vec_s = last_s[marks[4]]
        d_wq = main_s[:, :q_dim]
        d_wk = jnp.concatenate([main_s[:, q_dim:], rest_s[:, :q_dim + head_dim - width]], axis=1)
        d_wv = rest_s[:, q_dim + head_dim - width:]
        d_b, d_b1, d_b2 = vec_s[:w_rows], vec_s[w_rows:w_rows + f_rows], vec_s[w_rows + f_rows:w_rows + 2 * f_rows]

        attn_out = mm(attn_o, wo_b) + bo_f
        mlp_out = mm(act_b, wd_b) + bd_f
        x_out = (x_f + attn_out + mlp_out).astype(bf)[None]

        d_normed = mm_nt(dh_a, w12_a)
        d_normed_b = mm_nt(dh_b, w12_b)
        d_normed_q = mm_nt(dqkv_b, wqkv_b)
        d_normed = d_normed + d_normed_b + d_normed_q
        d_xf, d_scale = norm_back(d_normed)
        d_x = (grad_f + d_xf).astype(bf)[None]
        d_sc = scatter(d_scale[0])

        def up_grad(which):
            return jnp.concatenate([src[:, which * n * FT:(which + 1) * n * FT] for src, n in ((dw_a_s, tiles_of[0]), (dw_b_s, tiles_of[1]))], axis=1)

        return (x_out, d_x, d_sc, d_wq, d_wk, d_wv, d_wo, d_b, up_grad(0), d_b1, up_grad(1), d_b2, dwd_s, d_b)

    in_specs = (tok_spec, tok_spec, pos_spec, pos_spec) + param_specs
    out_specs = (tok_spec, tok_spec) + param_specs
    return jax.shard_map(local_step, mesh=mesh, in_specs=in_specs, out_specs=out_specs, check_vma=False)
```

```python
import functools
import jax
import jax.numpy as jnp
from jax import lax
from jax.experimental import pallas as pl
from jax.experimental.layout import Layout, with_layout_constraint
from jax.experimental.pallas import tpu as pltpu
from jax.sharding import PartitionSpec as P

WINDOW = 2048
ROPE_DIMS = 128
PARAM_AXES = ('cp', 'fsdp')
BQ = 256
BK = 256
FT = 256
VMEM_BYTES = 62 * 1024 * 1024
GELU_C = 0.7978845608028654
GELU_A = 0.044715


def rope_angle(seg_pos):
    half_dims = ROPE_DIMS // 2
    inv_freq = 10000.0 ** (-jnp.arange(half_dims, dtype=jnp.float32) / half_dims)
    return seg_pos.astype(jnp.float32)[..., None] * inv_freq


def rope_apply(values, cos_a, sin_a):
    half_dims = ROPE_DIMS // 2
    first_half = values[..., :half_dims]
    second_half = values[..., half_dims:ROPE_DIMS]
    return jnp.concatenate([first_half * cos_a - second_half * sin_a, second_half * cos_a + first_half * sin_a, values[..., ROPE_DIMS:]], axis=-1)


def rms_norm(x_f, scale_f):
    inv_rms = lax.rsqrt(jnp.mean(x_f * x_f, axis=-1, keepdims=True) + 1e-6)
    return x_f * inv_rms * (1.0 + scale_f)


def resident(shape):
    return pl.BlockSpec(shape, lambda *_: (0,) * len(shape), pipeline_mode=pl.Buffered(1))


def attn_kernel(n_heads, head_dim, lo_ref, q_ref, do_ref, cos_ref, sin_ref, kv_ref, kvt_ref, segk_ref, segq_ref, o_ref, dq_ref, dprev_ref, down_ref, q4, qt, do4, dot_, s_scr, dp_scr, dkv_ref):
    qb = pl.program_id(0)
    scale = head_dim ** -0.5
    cos_a = cos_ref[...]
    sin_a = sin_ref[...]

    def turn(vals, cos_v, sin_v):
        front = vals[:, :ROPE_DIMS]
        return jnp.concatenate([front * cos_v + pltpu.roll(front, ROPE_DIMS // 2, 1) * sin_v, vals[:, ROPE_DIMS:]], axis=1)

    @pl.when(qb == 0)
    def _():
        dkv_ref[...] = jnp.zeros_like(dkv_ref)

    for h in range(n_heads):
        cols = slice(h * head_dim, (h + 1) * head_dim)
        rows = slice(h * BQ, (h + 1) * BQ)
        q_f = turn(q_ref[:, cols], cos_a, sin_a)
        q_h = q_f.astype(jnp.bfloat16)
        do_h = do_ref[:, cols]
        q4[rows, :] = q_h
        do4[rows, :] = do_h
        qt[:, rows] = q_f.T.astype(jnp.bfloat16)
        dot_[:, rows] = do_h.astype(jnp.float32).T.astype(jnp.bfloat16)

    lo = lo_ref[qb]
    hi = (qb * BQ + BQ - 1 + WINDOW) // BK + 1
    segq = segq_ref[0]
    gap = lax.broadcasted_iota(jnp.int32, (BK, BQ), 1) - lax.broadcasted_iota(jnp.int32, (BK, BQ), 0)

    def k_rows(kb):
        return pl.ds(pl.multiple_of(kb * BK, BK), BK)

    def scores_step(kb, m):
        k_blk = kv_ref[k_rows(kb), :head_dim]
        dist = gap + (qb * BQ + WINDOW - kb * BK)
        allowed = (segk_ref[k_rows(kb), :] == segq) & (dist >= 0) & (dist < WINDOW)
        parts = []
        for h in range(n_heads):
            rows = slice(h * BQ, (h + 1) * BQ)
            s_h = jnp.dot(k_blk, qt[:, rows], preferred_element_type=jnp.float32) * scale
            s_h = jnp.where(allowed, s_h, -1e30)
            s_scr[kb - lo, :, rows] = s_h
            parts.append(jnp.maximum(m[h], jnp.max(s_h, axis=0, keepdims=True)))
        return tuple(parts)

    m = lax.fori_loop(lo, hi, scores_step, tuple(jnp.full((1, BQ), -1e30, jnp.float32) for _ in range(n_heads)))

    def exp_step(kb, carry):
        v_blk = kv_ref[k_rows(kb), head_dim:]
        sums, dots = [], []
        for h in range(n_heads):
            rows = slice(h * BQ, (h + 1) * BQ)
            dp_h = jnp.dot(v_blk, dot_[:, rows], preferred_element_type=jnp.float32)
            p_h = jnp.exp(s_scr[kb - lo, :, rows] - m[h])
            s_scr[kb - lo, :, rows] = p_h
            dp_scr[kb - lo, :, rows] = dp_h
            sums.append(carry[0][h] + jnp.sum(p_h, axis=0, keepdims=True))
            dots.append(carry[1][h] + jnp.sum(p_h * dp_h, axis=0, keepdims=True))
        return tuple(sums), tuple(dots)

    zeros = tuple(jnp.zeros((1, BQ), jnp.float32) for _ in range(n_heads))
    sums, dots = lax.fori_loop(lo, hi, exp_step, (zeros, zeros))
    inv_sum = [1.0 / sums[h] for h in range(n_heads)]
    delta = [dots[h] * inv_sum[h] for h in range(n_heads)]

    def grad_step(kb, carry):
        o_acc, dq_acc = carry
        cols = pl.ds(pl.multiple_of(kb * BK, BK), BK)
        kt_blk = kvt_ref[:head_dim, cols]
        vt_blk = kvt_ref[head_dim:, cols]
        p_parts, ds_parts = [], []
        for h in range(n_heads):
            rows = slice(h * BQ, (h + 1) * BQ)
            p_h = s_scr[kb - lo, :, rows] * inv_sum[h]
            ds_h = p_h * (dp_scr[kb - lo, :, rows] - delta[h]) * scale
            p_parts.append(p_h.astype(jnp.bfloat16))
            ds_parts.append(ds_h.astype(jnp.bfloat16))
        p_all = jnp.concatenate(p_parts, axis=1)
        ds_all = jnp.concatenate(ds_parts, axis=1)
        dkv_ref[k_rows(kb), :head_dim] += jnp.dot(ds_all, q4[...], preferred_element_type=jnp.float32)
        dkv_ref[k_rows(kb), head_dim:] += jnp.dot(p_all, do4[...], preferred_element_type=jnp.float32)
        o_acc = o_acc + jnp.dot(vt_blk, p_all, preferred_element_type=jnp.float32)
        dq_acc = dq_acc + jnp.dot(kt_blk, ds_all, preferred_element_type=jnp.float32)
        return o_acc, dq_acc

    wide = jnp.zeros((head_dim, n_heads * BQ), jnp.float32)
    o_acc, dq_acc = lax.fori_loop(lo, hi, grad_step, (wide, wide))
    for h in range(n_heads):
        cols = slice(h * head_dim, (h + 1) * head_dim)
        rows = slice(h * BQ, (h + 1) * BQ)
        o_ref[:, cols] = o_acc[:, rows].T.astype(jnp.bfloat16)
        dq_ref[:, cols] = turn(dq_acc[:, rows].T, cos_a, -sin_a).astype(jnp.bfloat16)

    @pl.when(qb == pl.num_programs(0) - 1)
    def _():
        dprev_ref[...] = dkv_ref[:WINDOW, :]
        down_ref[...] = dkv_ref[WINDOW:, :]


def attention(qkv, do_b, cos_a, sin_a, kv_all, seg_q, seg_all, n_heads):
    n_tok, q_dim = do_b.shape
    head_dim = q_dim // n_heads
    n_keys = kv_all.shape[0]
    n_q = n_tok // BQ
    n_span = WINDOW // BK + BQ // BK
    seg_first = seg_q.reshape(n_q, BQ)[:, 0]
    seg_last = seg_all.reshape(n_keys // BK, BK)[:, -1]
    first_seg_blk = jnp.sum((seg_last[None, :] < seg_first[:, None]).astype(jnp.int32), axis=1)
    first_win_blk = (jnp.arange(n_q, dtype=jnp.int32) * BQ + 1) // BK
    lo_blk = jnp.maximum(first_seg_blk, first_win_blk)
    wide = n_heads * BQ
    grid_spec = pltpu.PrefetchScalarGridSpec(
        num_scalar_prefetch=1,
        grid=(n_q,),
        in_specs=[
            pl.BlockSpec((BQ, q_dim), lambda i, lo: (i, 0)),
            pl.BlockSpec((BQ, q_dim), lambda i, lo: (i, 0)),
            pl.BlockSpec((BQ, ROPE_DIMS), lambda i, lo: (i, 0)),
            pl.BlockSpec((BQ, ROPE_DIMS), lambda i, lo: (i, 0)),
            resident((n_keys, 2 * head_dim)),
            resident((2 * head_dim, n_keys)),
            resident((n_keys, 1)),
            pl.BlockSpec((1, 1, BQ), lambda i, lo: (i, 0, 0)),
        ],
        out_specs=[
            pl.BlockSpec((BQ, q_dim), lambda i, lo: (i, 0)),
            pl.BlockSpec((BQ, q_dim), lambda i, lo: (i, 0)),
            resident((WINDOW, 2 * head_dim)),
            resident((n_keys - WINDOW, 2 * head_dim)),
        ],
        scratch_shapes=[
            pltpu.VMEM((wide, head_dim), jnp.bfloat16),
            pltpu.VMEM((head_dim, wide), jnp.bfloat16),
            pltpu.VMEM((wide, head_dim), jnp.bfloat16),
            pltpu.VMEM((head_dim, wide), jnp.bfloat16),
            pltpu.VMEM((n_span, BK, wide), jnp.float32),
            pltpu.VMEM((n_span, BK, wide), jnp.float32),
            pltpu.VMEM((n_keys, 2 * head_dim), jnp.float32),
        ],
    )
    return pl.pallas_call(
        functools.partial(attn_kernel, n_heads, head_dim),
        grid_spec=grid_spec,
        out_shape=(
            jax.ShapeDtypeStruct((n_tok, q_dim), jnp.bfloat16),
            jax.ShapeDtypeStruct((n_tok, q_dim), jnp.bfloat16),
            jax.ShapeDtypeStruct((WINDOW, 2 * head_dim), jnp.float32),
            jax.ShapeDtypeStruct((n_keys - WINDOW, 2 * head_dim), jnp.float32),
        ),
        compiler_params=pltpu.CompilerParams(dimension_semantics=('arbitrary',), vmem_limit_bytes=VMEM_BYTES),
        cost_estimate=pl.CostEstimate(flops=10 * n_tok * WINDOW * q_dim, bytes_accessed=40 << 20, transcendentals=n_tok * WINDOW * n_heads),
        name='attention',
    )(lo_blk, qkv, do_b, cos_a, sin_a, kv_all, kv_all.T, seg_all.reshape(n_keys, 1), seg_q.reshape(n_q, 1, BQ))


def act_kernel(n_tok, step_rows, n_ref, g_ref, nt_ref, w1_ref, w2_ref, wd_ref, b1_ref, b2_ref, *rest):
    act_ref, dh_ref, dw_ref, db_ref, d_two_scr, db_scr = rest[-6:]

    @pl.when(pl.program_id(1) == 0)
    def _():
        def one_tile(i, sums):
            rows = pl.ds(pl.multiple_of(i * step_rows, step_rows), step_rows)
            n_blk = n_ref[rows, :]
            h_one = jnp.dot(n_blk, w1_ref[...], preferred_element_type=jnp.float32) + b1_ref[...]
            h_two = jnp.dot(n_blk, w2_ref[...], preferred_element_type=jnp.float32) + b2_ref[...]
            d_act = lax.dot_general(g_ref[rows, :], wd_ref[...], (((1,), (1,)), ((), ())), preferred_element_type=jnp.float32)
            h_sq = h_one * h_one
            t = jnp.tanh(h_one * (GELU_C + (GELU_C * GELU_A) * h_sq))
            half = 0.5 + 0.5 * t
            gelu = h_one * half
            slope = half + (0.5 * h_one) * (1.0 - t * t) * (GELU_C + (3.0 * GELU_C * GELU_A) * h_sq)
            act_ref[rows, :] = (gelu * h_two).astype(jnp.bfloat16)
            d_one = d_act * h_two * slope
            d_two = d_act * gelu
            dh_ref[rows, :] = d_one.astype(jnp.bfloat16)
            d_two_scr[rows, :] = d_two.astype(jnp.bfloat16)
            return sums[0] + jnp.sum(d_one, axis=0, keepdims=True), sums[1] + jnp.sum(d_two, axis=0, keepdims=True)

        zero = jnp.zeros((1, FT), jnp.float32)
        s_one, s_two = lax.fori_loop(0, n_tok // step_rows, one_tile, (zero, zero), unroll=2)
        db_ref[...] = s_one
        db_scr[...] = s_two
        dw_ref[...] = jnp.dot(nt_ref[...], dh_ref[...], preferred_element_type=jnp.float32)

    @pl.when(pl.program_id(1) == 1)
    def _():
        dh_ref[...] = d_two_scr[...]
        db_ref[...] = db_scr[...]
        dw_ref[...] = jnp.dot(nt_ref[...], d_two_scr[...], preferred_element_type=jnp.float32)


def act_call(normed, normed_t, grad, w12, wd, b1, b2, act_buf, first_tile, n_tiles):
    n_tok, width = normed.shape
    ffn = wd.shape[0]
    in_specs = [
        resident((n_tok, width)),
        resident((n_tok, width)),
        resident((width, n_tok)),
        pl.BlockSpec((width, FT), lambda t, k: (0, t)),
        pl.BlockSpec((width, FT), lambda t, k: (0, t + n_tiles)),
        pl.BlockSpec((FT, width), lambda t, k: (t + first_tile, 0)),
        pl.BlockSpec((1, FT), lambda t, k: (0, t + first_tile)),
        pl.BlockSpec((1, FT), lambda t, k: (0, t + first_tile)),
    ]
    args = [normed, grad, normed_t, w12, w12, wd, b1, b2]
    alias = {}
    if act_buf is not None:
        in_specs.append(pl.BlockSpec(memory_space=pl.ANY))
        alias = {len(args): 0}
        args.append(act_buf)
    return pl.pallas_call(
        functools.partial(act_kernel, n_tok, 256),
        grid=(n_tiles, 2),
        in_specs=in_specs,
        out_specs=[
            pl.BlockSpec((n_tok, FT), lambda t, k: (0, t + first_tile)),
            pl.BlockSpec((n_tok, FT), lambda t, k: (0, t + k * n_tiles)),
            pl.BlockSpec((width, FT), lambda t, k: (0, t + k * n_tiles)),
            pl.BlockSpec((1, FT), lambda t, k: (0, t + k * n_tiles)),
        ],
        out_shape=(
            jax.ShapeDtypeStruct((n_tok, ffn), jnp.bfloat16),
            jax.ShapeDtypeStruct((n_tok, n_tiles * 2 * FT), jnp.bfloat16),
            jax.ShapeDtypeStruct((width, n_tiles * 2 * FT), jnp.float32),
            jax.ShapeDtypeStruct((1, n_tiles * 2 * FT), jnp.float32),
        ),
        scratch_shapes=[pltpu.VMEM((n_tok, FT), jnp.bfloat16), pltpu.VMEM((1, FT), jnp.float32)],
        input_output_aliases=alias,
        compiler_params=pltpu.CompilerParams(dimension_semantics=('arbitrary', 'arbitrary'), vmem_limit_bytes=VMEM_BYTES),
        cost_estimate=pl.CostEstimate(flops=10 * n_tok * width * FT * n_tiles, bytes_accessed=30 << 20, transcendentals=n_tok * FT * n_tiles),
        name='gated_act',
    )(*args)


def gather_kernel(n_arrays, *refs):
    srcs, outs = refs[:n_arrays], refs[n_arrays:2 * n_arrays]
    send_sem, recv_sem, own_sem = refs[2 * n_arrays:]
    fs, z = lax.axis_index('fsdp'), lax.axis_index('cp')
    here = (lax.rem(fs, 2), lax.rem(lax.div(fs, 2), 2), lax.div(fs, 4), z)

    def flip(piece):
        return [here[b] + (1 - 2 * here[b]) if b in piece else here[b] for b in range(4)]

    def slot_of(piece):
        bits = flip(piece)
        return bits[0] + 2 * bits[1] + 4 * bits[2] + 8 * bits[3]

    def device_of(axis):
        bits = flip((axis,))
        return {'cp': bits[3], 'fsdp': bits[0] + 2 * bits[1] + 4 * bits[2]}

    barrier = pltpu.get_barrier_semaphore()
    for axis in range(4):
        pl.semaphore_signal(barrier, inc=1, device_id=device_of(axis), device_id_type=pl.DeviceIdType.MESH)
    pl.semaphore_wait(barrier, 4)

    jobs = []
    for color in range(3):
        for a in range(n_arrays):
            total = srcs[a].shape[0]
            if total % 24 == 0:
                jobs.append((a, color, color * (total // 3), total // 3))
            elif color == 0:
                jobs.append((a, color, 0, total))
    copies = {}

    def copy_of(job, step, piece):
        key = (job, step, piece)
        if key not in copies:
            copies[key] = len(copies)
        return copies[key]

    def order_of(job):
        color = jobs[job][1]
        return [1 + (color + i) % 3 for i in range(3)] + [0]

    def make(job, step, piece, number, own):
        a, _, first, count = jobs[job]
        rows = pl.ds(first, count)
        slot = slot_of(piece)
        src = srcs[a].at[rows] if own else outs[a].at[slot, rows]
        return pltpu.make_async_remote_copy(src_ref=src, dst_ref=outs[a].at[slot, rows], send_sem=send_sem.at[number], recv_sem=recv_sem.at[number],
                                            device_id=device_of(order_of(job)[step]), device_id_type=pl.DeviceIdType.MESH)

    def send(job, step, piece):
        number = copy_of(job, step, piece)
        make(job, step, piece, number, piece == ()).start()

    def toggled(piece, axis):
        return tuple(sorted(set(piece) ^ {axis}))

    own_copies = []
    for a in range(n_arrays):
        own_copies.append(pltpu.make_async_copy(srcs[a], outs[a].at[slot_of(())], own_sem.at[a]))
        own_copies[-1].start()
    for step in range(4):
        for job in range(len(jobs)):
            send(job, step, ())
    held = {job: [()] for job in range(len(jobs))}
    for step in range(4):
        for job in range(len(jobs)):
            axis = order_of(job)[step]
            arrived = []
            for piece in held[job]:
                got = toggled(piece, axis)
                make(job, step, got, copy_of(job, step, piece), False).wait_recv()
                arrived.append(got)
                for later in range(step + 1, 4):
                    send(job, later, got)
            held[job] = held[job] + arrived
    for (job, step, piece), number in copies.items():
        make(job, step, piece, number, piece == ()).wait_send()
    for copy in own_copies:
        copy.wait()


def gather_first(n_dev, *pieces):
    n_jobs = sum(3 if piece.shape[0] % 24 == 0 else 1 for piece in pieces)
    sent = sum(piece.size * 2 * 7 for piece in pieces)
    return pl.pallas_call(
        functools.partial(gather_kernel, len(pieces)),
        in_specs=[pl.BlockSpec(memory_space=pltpu.VMEM)] * len(pieces),
        out_specs=[pl.BlockSpec(memory_space=pl.ANY)] * len(pieces),
        out_shape=[jax.ShapeDtypeStruct((n_dev,) + piece.shape, piece.dtype) for piece in pieces],
        scratch_shapes=[pltpu.SemaphoreType.DMA((15 * n_jobs,)), pltpu.SemaphoreType.DMA((15 * n_jobs,)), pltpu.SemaphoreType.DMA((len(pieces),))],
        compiler_params=pltpu.CompilerParams(collective_id=0, has_side_effects=True, vmem_limit_bytes=VMEM_BYTES),
        cost_estimate=pl.CostEstimate(flops=100 << 30, bytes_accessed=sent, transcendentals=0),
        name='gather_first',
    )(*pieces)


def mm(a, b):
    return jnp.dot(a, b, preferred_element_type=jnp.float32)


def mm_tn(a, b):
    return lax.dot_general(a, b, (((0,), (0,)), ((), ())), preferred_element_type=jnp.float32)


def mm_nt(a, b):
    return lax.dot_general(a, b, (((1,), (1,)), ((), ())), preferred_element_type=jnp.float32)


def solution(mesh):
    n_dev = mesh.shape['cp'] * mesh.shape['fsdp']
    tok_spec = P('fsdp', 'cp', None)
    pos_spec = P('fsdp', 'cp')
    vec_spec = P(PARAM_AXES)
    mat_spec = P(PARAM_AXES, None)
    param_specs = (vec_spec, mat_spec, mat_spec, mat_spec, mat_spec, vec_spec, mat_spec, vec_spec, mat_spec, vec_spec, mat_spec, vec_spec)
    fwd_pairs = [(0, 1)]
    back_pairs = [(1, 0)]

    def gather(piece):
        return lax.all_gather(piece, PARAM_AXES, axis=0, tiled=True)

    def scatter(full):
        return lax.psum_scatter(full, PARAM_AXES, scatter_dimension=0, tiled=True)

    def local_step(x_in, grad_out, seg_id, seg_pos, norm_scale, w_q, w_k, w_v, w_o, b_o, w_up1, b_up1, w_up2, b_up2, w_down, b_down):
        bf = jnp.bfloat16
        width = x_in.shape[2]
        head_dim = w_k.shape[1]
        q_dim = w_q.shape[1]
        n_heads = q_dim // head_dim
        ffn = w_up1.shape[1]
        n_tiles = ffn // FT
        tiles_of = (4 * n_tiles // 9, n_tiles - 4 * n_tiles // 9)
        starts = (0, tiles_of[0])
        w_rows, f_rows, e_rows = norm_scale.shape[0], b_up1.shape[0], w_o.shape[0]

        def up_part(c):
            cols = slice(starts[c] * FT, (starts[c] + tiles_of[c]) * FT)
            return jnp.concatenate([w_up1[:, cols].astype(bf), w_up2[:, cols].astype(bf)], axis=1)

        qkv_dim = q_dim + 2 * head_dim
        vec_piece = jnp.concatenate([norm_scale, b_o, b_down, b_up1, b_up2]).astype(bf)
        vec_piece = jnp.pad(vec_piece[None], ((0, 15), (0, width - vec_piece.shape[0])))
        w12_a, wd_b, vec_all = gather_first(n_dev, up_part(0), w_down.astype(bf), vec_piece)
        w12_a = w12_a.reshape(width, -1)
        wd_b = wd_b.reshape(ffn, width)
        attn_piece = jnp.concatenate([jnp.concatenate([w_q, w_k, w_v], axis=1).astype(bf), jnp.pad(w_o.astype(bf), ((0, 0), (0, qkv_dim - width)))], axis=0)
        attn_piece, up_b_piece, vec_all = lax.optimization_barrier((attn_piece, up_part(1), vec_all))
        attn_w = gather(attn_piece).reshape(n_dev, w_rows + e_rows, qkv_dim)
        w12_b = gather(up_b_piece)
        vec_all = vec_all[:, 0].astype(jnp.float32)
        offs = [0, w_rows, 2 * w_rows, 3 * w_rows, 3 * w_rows + f_rows, 3 * w_rows + 2 * f_rows]
        scale_f, bo_f, bd_f, b1_f, b2_f = [vec_all[:, offs[i]:offs[i + 1]].reshape(1, -1) for i in range(5)]

        wqkv_b = attn_w[:, :w_rows].reshape(width, qkv_dim)
        wo_b = attn_w[:, w_rows:, :width].reshape(q_dim, width)

        x_f = x_in[0].astype(jnp.float32)
        grad = grad_out[0]
        grad_f = grad.astype(jnp.float32)
        normed_f, norm_back = jax.vjp(rms_norm, x_f, scale_f)
        normed = with_layout_constraint(normed_f.astype(bf), Layout((0, 1)))
        normed_t = normed.T
        d_bias = jnp.sum(grad_f, axis=0, keepdims=True)
        rot_angle = rope_angle(seg_pos[0])
        cos_h, sin_h = jnp.cos(rot_angle), jnp.sin(rot_angle)
        cos_w = jnp.concatenate([cos_h, cos_h], axis=1)
        sin_w = jnp.concatenate([-sin_h, sin_h], axis=1)

        act_a, dh_a, dw_a, db_a = act_call(normed, normed_t, grad, w12_a, wd_b, b1_f, b2_f, None, starts[0], tiles_of[0])
        dw_a_s = scatter(dw_a)

        normed_q, db_a, d_bias = lax.optimization_barrier((normed, db_a, d_bias))
        qkv = with_layout_constraint(mm(normed_q, wqkv_b), Layout((0, 1)))
        kv_b = jnp.concatenate([rope_apply(qkv[:, q_dim:q_dim + head_dim], cos_h, sin_h).astype(bf), qkv[:, q_dim + head_dim:].astype(bf)], axis=1)
        kv_prev = lax.ppermute(kv_b, 'cp', fwd_pairs)
        seg_prev = lax.ppermute(seg_id[0], 'cp', fwd_pairs)
        do_b = mm_nt(grad, wo_b).astype(bf)

        act_b, dh_b, dw_b, db_b = act_call(normed_q, normed_t, grad, w12_b, wd_b, b1_f, b2_f, act_a, starts[1], tiles_of[1])
        dw_b_s = scatter(dw_b)

        kv_all = jnp.concatenate([kv_prev, kv_b], axis=0)
        seg_all = jnp.concatenate([seg_prev, seg_id[0]], axis=0)
        qkv, db_b = lax.optimization_barrier((qkv, db_b))
        attn_o, dq_b, d_prev, d_own = attention(qkv, do_b, cos_w, sin_w, kv_all, seg_id[0], seg_all, n_heads)
        d_kvl = d_own + lax.ppermute(d_prev, 'cp', back_pairs)

        act_b, dh_a, dh_b, attn_o = lax.optimization_barrier((act_b, dh_a, dh_b, attn_o))
        dwd = mm_tn(act_b, grad)
        dwo = mm_tn(attn_o, grad)
        dkv_b = jnp.concatenate([rope_apply(d_kvl[:, :head_dim], cos_h, -sin_h).astype(bf), d_kvl[:, head_dim:].astype(bf)], axis=1)
        dqkv_b = jnp.concatenate([dq_b, dkv_b], axis=1)
        dwqkv = lax.dot_general(normed_t, dqkv_b, (((1,), (0,)), ((), ())), preferred_element_type=jnp.float32)

        def bias_rows(which):
            part_a = db_a[:, which * tiles_of[0] * FT:(which + 1) * tiles_of[0] * FT]
            part_b = db_b[:, which * tiles_of[1] * FT:(which + 1) * tiles_of[1] * FT]
            return jnp.concatenate([part_a, part_b], axis=1).reshape(n_dev, f_rows)

        vec_rows = jnp.concatenate([d_bias.reshape(n_dev, w_rows), bias_rows(0), bias_rows(1)], axis=1)
        vec_rows = jnp.pad(vec_rows[:, None], ((0, 0), (0, 15), (0, width - vec_rows.shape[1])))
        rest_dim = qkv_dim - width
        fold = width // rest_dim
        dwqkv = dwqkv.reshape(n_dev, w_rows, qkv_dim)
        rest_rows = dwqkv[:, :, width:].reshape(n_dev, fold, w_rows // fold, rest_dim)
        rest_rows = jnp.concatenate([rest_rows[:, i] for i in range(fold)], axis=2)
        last = jnp.concatenate([dwd.reshape(n_dev, f_rows, width), dwo.reshape(n_dev, e_rows, width), dwqkv[:, :, :width], rest_rows, vec_rows], axis=1)
        last_s = scatter(last.reshape(-1, width))
        last_s = lax.optimization_barrier(last_s)
        marks = [0, f_rows, f_rows + e_rows, f_rows + e_rows + w_rows, f_rows + e_rows + w_rows + w_rows // fold]
        dwd_s, d_wo, main_s, rest_s = [last_s[marks[i]:marks[i + 1]] for i in range(4)]
        rest_s = jnp.concatenate([rest_s[:, i * rest_dim:(i + 1) * rest_dim] for i in range(fold)], axis=0)
        vec_s = last_s[marks[4]]
        d_wq = main_s[:, :q_dim]
        d_wk = jnp.concatenate([main_s[:, q_dim:], rest_s[:, :q_dim + head_dim - width]], axis=1)
        d_wv = rest_s[:, q_dim + head_dim - width:]
        d_b, d_b1, d_b2 = vec_s[:w_rows], vec_s[w_rows:w_rows + f_rows], vec_s[w_rows + f_rows:w_rows + 2 * f_rows]

        attn_out = mm(attn_o, wo_b) + bo_f
        mlp_out = mm(act_b, wd_b) + bd_f
        x_out = (x_f + attn_out + mlp_out).astype(bf)[None]

        d_normed = mm_nt(dh_a, w12_a)
        d_normed_b = mm_nt(dh_b, w12_b)
        d_normed_q = mm_nt(dqkv_b, wqkv_b)
        d_normed = d_normed + d_normed_b + d_normed_q
        d_xf, d_scale = norm_back(d_normed)
        d_x = (grad_f + d_xf).astype(bf)[None]
        d_sc = scatter(d_scale[0])

        def up_grad(which):
            return jnp.concatenate([src[:, which * n * FT:(which + 1) * n * FT] for src, n in ((dw_a_s, tiles_of[0]), (dw_b_s, tiles_of[1]))], axis=1)

        return (x_out, d_x, d_sc, d_wq, d_wk, d_wv, d_wo, d_b, up_grad(0), d_b1, up_grad(1), d_b2, dwd_s, d_b)

    in_specs = (tok_spec, tok_spec, pos_spec, pos_spec) + param_specs
    out_specs = (tok_spec, tok_spec) + param_specs
    return jax.shard_map(local_step, mesh=mesh, in_specs=in_specs, out_specs=out_specs, check_vma=False)
```
